512 devices in a mesh: row: 16 (over x, z_hi, core), vec: 32 (over z_lo, y).
Axes of the slice: x: 4, y: 4, z: 16 (z_hi: 2, z_lo: 8; z = z_hi * 8 + z_lo), core: 2. Of those that a mesh axis runs over, the one named last changes fastest.
Arguments:
- old_vectors: float32 [640, 49152], P('vec', 'row'), may hold values from -6 to 6
- panel_source: int32 [256], replicated, may hold values from 0 to 639, as said below
- secular: float32 [4096, 256], P('vec'), may hold values from -0.375 to 0.375
- reflectors: float32 [256, 49152], P('vec', 'row'), may hold values from -6 to 6
- wy_factor: float32 [256, 256], replicated, as said below
- cholesky_panel: float32 [256, 49152], P('vec', 'row'), may hold values from -0.02734375 to 0.02734375
- panel_inverse: float32 [256, 256], replicated, as said below
Outputs:
- vectors: float32 [4096, 49152], P('vec', 'row')
The draws below stay inside these ranges and needn't reach their ends.
Inputs may be any that keep to these rules, and one draw needn't show every extreme that they name: `panel_source`: distinct numbers; each block of 20 consecutive old vectors (those of one index of vec) supplies at most 12 panel columns, and some block supplies exactly 12. `wy_factor`: upper triangular. `panel_inverse`: upper triangular.
All inputs are finite; a program needn't handle non-finite values.
Results may differ from the reference program's by a relative error of at most 0.0001.
Values sent between devices are 32-bit elements; how exact they have to be, the bound alone decides.
No kernel may reach another device: no remote copies, remote signals or barrier semaphores. Data moves between devices by JAX's collectives and lax.ppermute only.
A program may use at most 64 MiB of HBM per device.

```python
import jax
import jax.numpy as jnp
from jax import lax

PANEL = 256
MAXC = 12
QV_DEV = 20
OLDV = 640
ORDER = 49152
VECTORS = 4096


def draw_panel_source(key, part):
    subkeys = jax.random.split(jax.random.fold_in(key, 11), 4)
    blocks = OLDV // QV_DEV
    scores = jax.random.randint(subkeys[0], (blocks, QV_DEV), 0, 1 << 30)
    local_pick = jnp.argsort(scores, axis=1, stable=True)[:, :MAXC].astype(jnp.int32)
    candidates = (local_pick + QV_DEV * jnp.arange(blocks, dtype=jnp.int32)[:, None]).reshape(-1)
    busiest = jax.random.randint(subkeys[1], (), 0, blocks)
    block_of = jnp.repeat(jnp.arange(blocks, dtype=jnp.int32), MAXC)
    priority = jax.random.randint(subkeys[2], (blocks * MAXC,), 0, 1 << 20) + jnp.where(block_of == busiest, 1 << 21, 0)
    ranking = jnp.argsort(-priority, stable=True)
    chosen = candidates[ranking[:PANEL]]
    return jax.random.permutation(subkeys[3], chosen).astype(jnp.int32)


def draw_wy_factor(key, part):
    subkeys = jax.random.split(jax.random.fold_in(key, 23), 2)
    diagonal = jax.random.uniform(subkeys[0], (PANEL,), jnp.float32, 1.0, 2.0)
    off_diagonal = jax.random.normal(subkeys[1], (PANEL, PANEL), jnp.float32) / jnp.sqrt(jnp.float32(PANEL))
    matrix = jnp.triu(off_diagonal, 1) + jnp.diag(diagonal)
    return 4.0 / ORDER * matrix


def draw_panel_inverse(key, part):
    subkeys = jax.random.split(jax.random.fold_in(key, 37), 2)
    diagonal = jnp.exp(jax.random.uniform(subkeys[0], (PANEL,), jnp.float32, -0.7, 0.7))
    off_diagonal = 0.6 * jax.random.normal(subkeys[1], (PANEL, PANEL), jnp.float32) / jnp.sqrt(jnp.float32(PANEL))
    return jnp.triu(off_diagonal, 1) + jnp.diag(diagonal)


def block_levels(stream_key, dims, shards, smallest, high):
    def one(axis_at, blocks):
        steps = jax.random.uniform(jax.random.fold_in(jax.random.fold_in(stream_key, 6), axis_at), (blocks,), jnp.float32, smallest / len(shards), high / len(shards))
        return jnp.repeat(jnp.exp(steps), dims[axis_at] // blocks).reshape((-1,) + (1,) * (len(dims) - axis_at - 1))

    factor_of = one(*shards[0])
    for cut in shards[1:]:
        factor_of = factor_of * one(*cut)
    return factor_of


def scatter_about(stream_key, shape, spread, most, shards=(), held_as=jnp.bfloat16):
    drawn = spread * jax.random.normal(stream_key, shape, jnp.float32)
    if shards:
        drawn = drawn * block_levels(stream_key, shape, shards, -0.22, 0.18)
    return jnp.clip(drawn, -most, most).astype(held_as)


def setup_inputs(seed: int = 0) -> dict:
    key_list = jax.random.split(jax.random.key(seed), 8)
    return {
        "old_vectors": scatter_about(key_list[0], (OLDV, ORDER), 1.0, 6.0, ((0, 32), (1, 16)), jnp.float32),
        "panel_source": draw_panel_source(jax.random.fold_in(key_list[7], 71), 0),
        "secular": scatter_about(key_list[2], (VECTORS, PANEL), PANEL ** -0.5, 0.375, ((0, 32),), jnp.float32),
        "reflectors": scatter_about(key_list[3], (PANEL, ORDER), 1.0, 6.0, ((0, 32), (1, 16)), jnp.float32),
        "wy_factor": draw_wy_factor(jax.random.fold_in(key_list[7], 71), 0),
        "cholesky_panel": scatter_about(key_list[5], (PANEL, ORDER), ORDER ** -0.5, 0.02734375, ((0, 32), (1, 16)), jnp.float32),
        "panel_inverse": draw_panel_inverse(jax.random.fold_in(key_list[7], 71), 0),
    }


def product(left, right):
    return jnp.dot(left, right, precision=lax.Precision.HIGHEST, preferred_element_type=jnp.float32)


def reference(old_vectors, panel_source, secular, reflectors, wy_factor, cholesky_panel, panel_inverse):
    picked = jnp.take(old_vectors, panel_source, axis=0)
    merged = product(secular, picked)
    inner_products = product(merged, reflectors.T)
    wy_coeff = product(inner_products, wy_factor.T)
    applied = merged - product(wy_coeff, reflectors)
    correction = product(applied[:, PANEL:], cholesky_panel[:, PANEL:].T)
    top_rows = product(applied[:, :PANEL] - correction, panel_inverse.T)
    return jnp.concatenate([top_rows, applied[:, PANEL:]], axis=1)
```

```python
import jax
import jax.numpy as jnp
from jax import lax
from jax.sharding import Mesh
from jax.sharding import PartitionSpec as P

VEC = ("z", "y")
HOPS = (4, 2, 1)


def product(left, right, contract=(1, 0)):
    return lax.dot_general(
        left,
        right,
        (((contract[0],), (contract[1],)), ((), ())),
        precision=lax.Precision.HIGHEST,
        preferred_element_type=jnp.float32,
    )


def onehot(index, width):
    return (index[:, None] == jnp.arange(width, dtype=jnp.int32)[None, :]).astype(jnp.float32)


def doubled(block, axis, hops):
    width = lax.axis_size(axis)
    for hop in hops:
        other = lax.ppermute(block, axis, [(i, i ^ hop) for i in range(width)])
        block = jnp.concatenate([block, other], axis=0)
    return block


def place_of(index, mine, hops):
    apart = index ^ mine
    return sum(((apart // hop) % 2) << k for k, hop in enumerate(hops))


def scattered_sum(parts, axis):
    return jnp.sum(lax.all_to_all(parts, axis, 0, 0), axis=0)


def spread(array, axis):
    copies = jnp.broadcast_to(array[None], (lax.axis_size(axis), *array.shape))
    return lax.all_to_all(copies, axis, 0, 0)


def summed_rows(partial, groups):
    rows, width = partial.shape
    own = scattered_sum(partial.reshape(groups, rows // groups, width), "y")
    own = jnp.sum(spread(own, "row"), axis=0)
    return spread(own, VEC).reshape(-1, width)


def per_device(
    old_vectors, panel_source, secular, reflectors, wy_factor, cholesky_panel, panel_inverse
):
    panel = secular.shape[1]
    old_count, row_count = old_vectors.shape
    z_width, y_width = lax.axis_size("z"), lax.axis_size("y")
    vec_width = z_width * y_width
    z_index, y_index = lax.axis_index("z"), lax.axis_index("y")
    row_index = lax.axis_index("row")
    share = panel // vec_width
    slots = 3 * share // 2
    cols = row_count // y_width

    owner = panel_source // old_count
    local = panel_source % old_count
    order = jnp.arange(panel, dtype=jnp.int32)
    same = (owner[:, None] == owner[None, :]) & (order[:, None] > order[None, :])
    earlier = jnp.sum(same.astype(jnp.int32), axis=1)
    mine = owner == z_index * y_width + y_index
    picker = (
        (earlier[None, :] == jnp.arange(slots, dtype=jnp.int32)[:, None]) & mine[None, :]
    ).astype(jnp.float32)
    chooser = product(picker, onehot(local, old_count))
    buffer = product(chooser, old_vectors)

    packed = jnp.concatenate([reflectors, cholesky_panel, buffer], axis=0)
    packed = packed.reshape(packed.shape[0], y_width, cols).transpose(1, 0, 2)
    packed = lax.all_to_all(packed, "y", 0, 0)
    own_reflectors = packed[:, :share].reshape(-1, cols)
    own_cholesky = packed[:, share : 2 * share].reshape(-1, cols)
    own_slots = packed[:, 2 * share :].reshape(-1, cols)
    first = row_index * row_count + y_index * cols
    below = first + jnp.arange(cols, dtype=jnp.int32) >= panel
    own_cholesky = jnp.where(below[None, :], own_cholesky, 0.0)

    all_reflectors = doubled(own_reflectors, "z", HOPS)
    all_slots = doubled(own_slots, "z", HOPS)

    group = share * y_width
    turned = onehot(place_of(order // group, z_index, HOPS) * group + order % group, panel)
    inner = product(product(own_slots, all_reflectors, (1, 1)), turned, (1, 1))
    inner = summed_rows(inner, y_width)
    inner = product(onehot(owner * slots + earlier, slots * vec_width), inner)
    coeff = product(inner, product(wy_factor, turned, (0, 0)))

    z_place = place_of(owner // y_width, z_index, HOPS)
    held_at = (z_place * y_width + owner % y_width) * slots + earlier
    gathered = product(onehot(held_at, slots * vec_width), all_slots)
    transformed = gathered - product(coeff, all_reflectors)

    blocks = [transformed] + [
        lax.ppermute(transformed, "y", [(i, (i + d) % y_width) for i in range(y_width)])
        for d in range(1, y_width)
    ]
    cross = summed_rows(product(own_cholesky, transformed, (1, 1)), y_width)
    correction = product(secular, cross, (1, 1))

    applied = jnp.zeros((secular.shape[0], row_count), jnp.float32)
    for d, block in enumerate(blocks):
        at = ((y_index - d + y_width) % y_width) * cols
        applied = lax.dynamic_update_slice(applied, product(secular, block), (0, at))
    head = applied[:, :panel]
    solved = product(head - correction, panel_inverse, (1, 1))
    return lax.dynamic_update_slice(applied, jnp.where(row_index == 0, solved, head), (0, 0))


def solution(mesh):
    split = Mesh(mesh.devices.reshape(mesh.shape["row"], 8, 4), ("row", "z", "y"))
    return jax.shard_map(
        per_device,
        mesh=split,
        in_specs=(P(VEC, "row"), P(), P(VEC, None), P(VEC, "row"), P(), P(VEC, "row"), P()),
        out_specs=P(VEC, "row"),
        check_vma=False,
    )
```

```python
import jax
import jax.numpy as jnp
from jax import lax
from jax.sharding import Mesh
from jax.sharding import PartitionSpec as P


ROW = ("x", "zh", "core")
VEC = ("z", "y")
HOPS = (4, 2, 1)


def product(left, right, contract=(1, 0)):
    return lax.dot_general(
        left,
        right,
        (((contract[0],), (contract[1],)), ((), ())),
        precision=lax.Precision.HIGHEST,
        preferred_element_type=jnp.float32,
    )


def onehot(index, width):
    return (index[:, None] == jnp.arange(width, dtype=jnp.int32)[None, :]).astype(jnp.float32)


def doubled(block, axis, hops):
    width = lax.axis_size(axis)
    for hop in hops:
        other = lax.ppermute(block, axis, [(i, i ^ hop) for i in range(width)])
        block = jnp.concatenate([block, other], axis=0)
    return block


def place_of(index, mine, hops):
    apart = index ^ mine
    return sum(((apart // hop) % 2) << k for k, hop in enumerate(hops))


def spread(array, axis):
    copies = jnp.broadcast_to(array[None], (lax.axis_size(axis), *array.shape))
    return lax.all_to_all(copies, axis, 0, 0)


def summed_rows(partial):
    parts = partial.reshape(lax.axis_size("y"), -1, partial.shape[1])
    group = lax.axis_size("x") * lax.axis_size("core")
    parts = jnp.broadcast_to(parts[None], (group, *parts.shape)).reshape(-1, *parts.shape[1:])
    parts = lax.all_to_all(parts, ("x", "core", "y"), 0, 0)
    own = jnp.sum(parts, axis=0)
    own = own + lax.ppermute(own, "zh", [(0, 1), (1, 0)])
    return spread(spread(own, "z"), "y")


def per_device(
    old_vectors, panel_source, secular, reflectors, wy_factor, cholesky_panel, panel_inverse
):
    panel = secular.shape[1]
    old_count, row_count = old_vectors.shape
    z_width, y_width = lax.axis_size("z"), lax.axis_size("y")
    vec_width = z_width * y_width
    z_index, y_index = lax.axis_index("z"), lax.axis_index("y")
    row_index = lax.axis_index(ROW)
    share = panel // vec_width
    slots = 3 * share // 2
    cols = row_count // y_width

    owner = panel_source // old_count
    local = panel_source % old_count
    order = jnp.arange(panel, dtype=jnp.int32)
    same = (owner[:, None] == owner[None, :]) & (order[:, None] > order[None, :])
    earlier = jnp.sum(same.astype(jnp.int32), axis=1)
    mine = owner == z_index * y_width + y_index
    picker = (
        (earlier[None, :] == jnp.arange(slots, dtype=jnp.int32)[:, None]) & mine[None, :]
    ).astype(jnp.float32)
    chooser = product(picker, onehot(local, old_count))
    buffer = product(chooser, old_vectors)

    packed = jnp.concatenate([reflectors, cholesky_panel, buffer], axis=0)
    packed = packed.reshape(packed.shape[0], y_width, cols).transpose(1, 0, 2)
    packed = lax.all_to_all(packed, "y", 0, 0)
    own_reflectors = packed[:, :share].reshape(-1, cols)
    own_cholesky = packed[:, share : 2 * share].reshape(-1, cols)
    own_slots = packed[:, 2 * share :].reshape(-1, cols)
    first = row_index * row_count + y_index * cols
    below = first + jnp.arange(cols, dtype=jnp.int32) >= panel
    own_cholesky = jnp.where(below[None, :], own_cholesky, 0.0)

    all_reflectors = doubled(own_reflectors, "z", HOPS)
    all_slots = doubled(own_slots, "z", HOPS)

    group = share * y_width
    turned = onehot(place_of(order // group, z_index, HOPS) * group + order % group, panel)
    inner = product(product(own_slots, all_reflectors, (1, 1)), turned, (1, 1))
    inner = summed_rows(inner).reshape(-1, panel)
    summed_at = ((owner % y_width) * z_width + owner // y_width) * slots + earlier
    inner = product(onehot(summed_at, slots * vec_width), inner)
    coeff = product(inner, product(wy_factor, turned, (0, 0)))

    z_place = place_of(owner // y_width, z_index, HOPS)
    held_at = (z_place * y_width + owner % y_width) * slots + earlier
    gathered = product(onehot(held_at, slots * vec_width), all_slots)
    transformed = gathered - product(coeff, all_reflectors)

    blocks = [transformed]
    for d in range(1, y_width):
        turn = [(i, (i + d) % y_width) for i in range(y_width)]
        blocks.append(lax.ppermute(transformed, "y", turn))
    cross = summed_rows(product(own_cholesky, transformed, (1, 1)))
    cross = cross.transpose(1, 0, 2, 3).reshape(-1, panel)
    correction = product(secular, cross, (1, 1))

    applied = jnp.zeros((secular.shape[0], row_count), jnp.float32)
    for d, block in enumerate(blocks):
        at = ((y_index - d + y_width) % y_width) * cols
        applied = lax.dynamic_update_slice(applied, product(secular, block), (0, at))
    head = applied[:, :panel]
    solved = product(head - correction, panel_inverse, (1, 1))
    return lax.dynamic_update_slice(applied, jnp.where(row_index == 0, solved, head), (0, 0))


def solution(mesh):
    split = Mesh(mesh.devices.reshape(mesh.shape["row"] // 4, 2, 2, 8, 4), ROW + VEC)

    return jax.shard_map(
        per_device,
        mesh=split,
        in_specs=(P(VEC, ROW), P(), P(VEC, None), P(VEC, ROW), P(), P(VEC, ROW), P()),
        out_specs=P(VEC, ROW),
        check_vma=False,
    )
```

```python
import jax
import jax.numpy as jnp
from jax import lax
from jax.sharding import Mesh
from jax.sharding import PartitionSpec as P


ROW = ("x", "zh", "core")
VEC = ("z", "y")
HOPS = (4, 2, 1)


def product(left, right, contract=(1, 0)):
    return lax.dot_general(
        left,
        right,
        (((contract[0],), (contract[1],)), ((), ())),
        precision=lax.Precision.HIGHEST,
        preferred_element_type=jnp.float32,
    )


def onehot(index, width):
    return (index[:, None] == jnp.arange(width, dtype=jnp.int32)[None, :]).astype(jnp.float32)


def doubled(block, axis, hops):
    width = lax.axis_size(axis)
    for hop in hops:
        other = lax.ppermute(block, axis, [(i, i ^ hop) for i in range(width)])
        block = jnp.concatenate([block, other], axis=0)
    return block


def place_of(index, mine, hops):
    apart = index ^ mine
    return sum(((apart // hop) % 2) << k for k, hop in enumerate(hops))


def spread(array, axis):
    copies = jnp.broadcast_to(array[None], (lax.axis_size(axis), *array.shape))
    return lax.all_to_all(copies, axis, 0, 0)


def summed_rows(partial):
    parts = partial.reshape(lax.axis_size("y"), -1, partial.shape[1])
    group = lax.axis_size("x") * lax.axis_size("core")
    parts = jnp.broadcast_to(parts[None], (group, *parts.shape)).reshape(-1, *parts.shape[1:])
    parts = lax.all_to_all(parts, ("x", "core", "y"), 0, 0)
    own = jnp.sum(parts, axis=0)
    halves = spread(own, ("zh", "z"))
    halves = halves.reshape(lax.axis_size("zh"), -1, *own.shape)
    column = jnp.sum(halves, axis=0)
    return spread(column, "y")


def per_device(
    old_vectors, panel_source, secular, reflectors, wy_factor, cholesky_panel, panel_inverse
):
    panel = secular.shape[1]
    old_count, row_count = old_vectors.shape
    z_width, y_width = lax.axis_size("z"), lax.axis_size("y")
    vec_width = z_width * y_width
    z_index, y_index = lax.axis_index("z"), lax.axis_index("y")
    row_index = lax.axis_index(ROW)
    share = panel // vec_width
    slots = 3 * share // 2
    cols = row_count // y_width

    owner = panel_source // old_count
    local = panel_source % old_count
    order = jnp.arange(panel, dtype=jnp.int32)
    same = (owner[:, None] == owner[None, :]) & (order[:, None] > order[None, :])
    earlier = jnp.sum(same.astype(jnp.int32), axis=1)
    mine = owner == z_index * y_width + y_index
    picker = (
        (earlier[None, :] == jnp.arange(slots, dtype=jnp.int32)[:, None]) & mine[None, :]
    ).astype(jnp.float32)
    chooser = product(picker, onehot(local, old_count))
    buffer = product(chooser, old_vectors)

    packed = jnp.concatenate([reflectors, cholesky_panel, buffer], axis=0)
    packed = packed.reshape(packed.shape[0], y_width, cols).transpose(1, 0, 2)
    packed = lax.all_to_all(packed, "y", 0, 0)
    own_reflectors = packed[:, :share].reshape(-1, cols)
    own_cholesky = packed[:, share : 2 * share].reshape(-1, cols)
    own_slots = packed[:, 2 * share :].reshape(-1, cols)
    first = row_index * row_count + y_index * cols
    below = first + jnp.arange(cols, dtype=jnp.int32) >= panel
    own_cholesky = jnp.where(below[None, :], own_cholesky, 0.0)

    all_reflectors = doubled(own_reflectors, "z", HOPS)
    all_slots = doubled(own_slots, "z", HOPS)

    group = share * y_width
    turned = onehot(place_of(order // group, z_index, HOPS) * group + order % group, panel)
    inner = product(product(own_slots, all_reflectors, (1, 1)), turned, (1, 1))
    inner = summed_rows(inner).reshape(-1, panel)
    summed_at = ((owner % y_width) * z_width + owner // y_width) * slots + earlier
    inner = product(onehot(summed_at, slots * vec_width), inner)
    coeff = product(inner, product(wy_factor, turned, (0, 0)))

    z_place = place_of(owner // y_width, z_index, HOPS)
    held_at = (z_place * y_width + owner % y_width) * slots + earlier
    gathered = product(onehot(held_at, slots * vec_width), all_slots)
    transformed = gathered - product(coeff, all_reflectors)

    blocks = [transformed]
    for d in range(1, y_width):
        turn = [(i, (i + d) % y_width) for i in range(y_width)]
        blocks.append(lax.ppermute(transformed, "y", turn))
    cross = summed_rows(product(own_cholesky, transformed, (1, 1)))
    cross = cross.transpose(1, 0, 2, 3).reshape(-1, panel)
    correction = product(secular, cross, (1, 1))

    applied = jnp.zeros((secular.shape[0], row_count), jnp.float32)
    for d, block in enumerate(blocks):
        at = ((y_index - d + y_width) % y_width) * cols
        applied = lax.dynamic_update_slice(applied, product(secular, block), (0, at))
    head = applied[:, :panel]
    solved = product(head - correction, panel_inverse, (1, 1))
    return lax.dynamic_update_slice(applied, jnp.where(row_index == 0, solved, head), (0, 0))


def solution(mesh):
    split = Mesh(mesh.devices.reshape(mesh.shape["row"] // 4, 2, 2, 8, 4), ROW + VEC)

    return jax.shard_map(
        per_device,
        mesh=split,
        in_specs=(P(VEC, ROW), P(), P(VEC, None), P(VEC, ROW), P(), P(VEC, ROW), P()),
        out_specs=P(VEC, ROW),
        check_vma=False,
    )
```

```python
import jax
import jax.numpy as jnp
from jax import lax
from jax.sharding import Mesh
from jax.sharding import PartitionSpec as P


ROW = ("x", "zh", "core")
VEC = ("z", "y")
HOPS = (4, 2, 1)


def product(left, right, contract=(1, 0)):
    return lax.dot_general(
        left,
        right,
        (((contract[0],), (contract[1],)), ((), ())),
        precision=lax.Precision.HIGHEST,
        preferred_element_type=jnp.float32,
    )


def onehot(index, width):
    return (index[:, None] == jnp.arange(width, dtype=jnp.int32)[None, :]).astype(jnp.float32)


def doubled(block, axis, hops):
    width = lax.axis_size(axis)
    for hop in hops:
        other = lax.ppermute(block, axis, [(i, i ^ hop) for i in range(width)])
        block = jnp.concatenate([block, other], axis=0)
    return block


def place_of(index, mine, hops):
    apart = index ^ mine
    return sum(((apart // hop) % 2) << k for k, hop in enumerate(hops))


def spread(array, axis):
    copies = jnp.broadcast_to(array[None], (lax.axis_size(axis), *array.shape))
    return lax.all_to_all(copies, axis, 0, 0)


def summed_rows(partial):
    parts = partial.reshape(lax.axis_size("y"), -1, partial.shape[1])
    group = lax.axis_size("x") * lax.axis_size("core")
    parts = jnp.broadcast_to(parts[None], (group, *parts.shape)).reshape(-1, *parts.shape[1:])
    parts = lax.all_to_all(parts, ("x", "core", "y"), 0, 0)
    own = jnp.sum(parts, axis=0)
    halves = spread(own, ("zh", "z"))
    halves = halves.reshape(lax.axis_size("zh"), -1, *own.shape)
    column = jnp.sum(halves, axis=0)
    return spread(column, "y")


def per_device(
    old_vectors, panel_source, secular, reflectors, wy_factor, cholesky_panel, panel_inverse
):
    panel = secular.shape[1]
    old_count, row_count = old_vectors.shape
    z_width, y_width = lax.axis_size("z"), lax.axis_size("y")
    vec_width = z_width * y_width
    z_index, y_index = lax.axis_index("z"), lax.axis_index("y")
    row_index = lax.axis_index(ROW)
    share = panel // vec_width
    slots = 3 * share // 2
    cols = row_count // y_width

    owner = panel_source // old_count
    local = panel_source % old_count
    order = jnp.arange(panel, dtype=jnp.int32)
    same = (owner[:, None] == owner[None, :]) & (order[:, None] > order[None, :])
    earlier = jnp.sum(same.astype(jnp.int32), axis=1)
    mine = owner == z_index * y_width + y_index
    picker = (
        (earlier[None, :] == jnp.arange(slots, dtype=jnp.int32)[:, None]) & mine[None, :]
    ).astype(jnp.float32)
    chooser = product(picker, onehot(local, old_count))
    buffer = product(chooser, old_vectors)

    packed = jnp.concatenate([reflectors, cholesky_panel, buffer], axis=0)
    packed = packed.reshape(packed.shape[0], y_width, cols).transpose(1, 0, 2)
    packed = lax.all_to_all(packed, "y", 0, 0)
    own_reflectors = packed[:, :share].reshape(-1, cols)
    own_cholesky = packed[:, share : 2 * share].reshape(-1, cols)
    own_slots = packed[:, 2 * share :].reshape(-1, cols)
    first = row_index * row_count + y_index * cols
    below = first + jnp.arange(cols, dtype=jnp.int32) >= panel
    own_cholesky = jnp.where(below[None, :], own_cholesky, 0.0)

    all_reflectors = doubled(own_reflectors, "z", HOPS)
    all_slots = doubled(own_slots, "z", HOPS)

    group = share * y_width
    turned = onehot(place_of(order // group, z_index, HOPS) * group + order % group, panel)
    inner = product(product(own_slots, all_reflectors, (1, 1)), turned, (1, 1))
    inner = summed_rows(inner).reshape(-1, panel)
    summed_at = ((owner % y_width) * z_width + owner // y_width) * slots + earlier
    inner = product(onehot(summed_at, slots * vec_width), inner)
    coeff = product(inner, product(wy_factor, turned, (0, 0)))

    z_place = place_of(owner // y_width, z_index, HOPS)
    held_at = (z_place * y_width + owner % y_width) * slots + earlier
    gathered = product(onehot(held_at, slots * vec_width), all_slots)
    transformed = gathered - product(coeff, all_reflectors)

    ahead = [(i, (i + 1) % y_width) for i in range(y_width)]
    behind = [(i, (i - 1) % y_width) for i in range(y_width)]
    before = lax.ppermute(transformed, "y", ahead)
    after = lax.ppermute(transformed, "y", behind)
    upper = lax.ppermute(before[: panel // 2], "y", ahead)
    lower = lax.ppermute(after[panel // 2 :], "y", behind)
    blocks = [(0, transformed), (1, before), (-1, after), (2, jnp.concatenate([upper, lower], axis=0))]
    cross = summed_rows(product(own_cholesky, transformed, (1, 1)))
    cross = cross.transpose(1, 0, 2, 3).reshape(-1, panel)
    correction = product(secular, cross, (1, 1))

    applied = jnp.zeros((secular.shape[0], row_count), jnp.float32)
    for d, block in blocks:
        at = ((y_index - d + y_width) % y_width) * cols
        applied = lax.dynamic_update_slice(applied, product(secular, block), (0, at))
    head = applied[:, :panel]
    solved = product(head - correction, panel_inverse, (1, 1))
    return lax.dynamic_update_slice(applied, jnp.where(row_index == 0, solved, head), (0, 0))


def solution(mesh):
    split = Mesh(mesh.devices.reshape(mesh.shape["row"] // 4, 2, 2, 8, 4), ROW + VEC)

    return jax.shard_map(
        per_device,
        mesh=split,
        in_specs=(P(VEC, ROW), P(), P(VEC, None), P(VEC, ROW), P(), P(VEC, ROW), P()),
        out_specs=P(VEC, ROW),
        check_vma=False,
    )
```

```python
import jax
import jax.numpy as jnp
from jax import lax
from jax.experimental import pallas as pl
from jax.experimental.pallas import tpu as pltpu
from jax.sharding import Mesh
from jax.sharding import PartitionSpec as P


ROW = ("x", "zh", "core")
VEC = ("z", "y")
HOPS = (4, 2, 1)


def product(left, right, contract=(1, 0)):
    return lax.dot_general(
        left,
        right,
        (((contract[0],), (contract[1],)), ((), ())),
        precision=lax.Precision.HIGHEST,
        preferred_element_type=jnp.float32,
    )


def onehot(index, width):
    return (index[:, None] == jnp.arange(width, dtype=jnp.int32)[None, :]).astype(jnp.float32)


def doubled(block, axis, hops):
    width = lax.axis_size(axis)
    for hop in hops:
        other = lax.ppermute(block, axis, [(i, i ^ hop) for i in range(width)])
        block = jnp.concatenate([block, other], axis=0)
    return block


def place_of(index, mine, hops):
    apart = index ^ mine
    return sum(((apart // hop) % 2) << k for k, hop in enumerate(hops))


def spread(array, axis):
    copies = jnp.broadcast_to(array[None], (lax.axis_size(axis), *array.shape))
    return lax.all_to_all(copies, axis, 0, 0)


def summed_rows(partial):
    parts = partial.reshape(lax.axis_size("y"), -1, partial.shape[-1])
    group = lax.axis_size("x") * lax.axis_size("core")
    parts = jnp.broadcast_to(parts[None], (group, *parts.shape)).reshape(-1, *parts.shape[1:])
    parts = lax.all_to_all(parts, ("x", "core", "y"), 0, 0)
    own = jnp.sum(parts, axis=0)
    halves = spread(own, ("zh", "z"))
    halves = halves.reshape(lax.axis_size("zh"), -1, *own.shape)
    column = jnp.sum(halves, axis=0)
    return spread(column, "y")


def named_permute(array, pairs):
    return lax.ppermute(array, "y", pairs)


def per_device(
    old_vectors, panel_source, secular, reflectors, wy_factor, cholesky_panel, panel_inverse
):
    panel = secular.shape[1]
    old_count, row_count = old_vectors.shape
    z_width, y_width = lax.axis_size("z"), lax.axis_size("y")
    vec_width = z_width * y_width
    z_index, y_index = lax.axis_index("z"), lax.axis_index("y")
    row_index = lax.axis_index(ROW)
    share = panel // vec_width
    slots = 3 * share // 2
    cols = row_count // y_width

    owner = panel_source // old_count
    local = panel_source % old_count
    order = jnp.arange(panel, dtype=jnp.int32)
    same = (owner[:, None] == owner[None, :]) & (order[:, None] > order[None, :])
    earlier = jnp.sum(same.astype(jnp.int32), axis=1)
    mine = owner == z_index * y_width + y_index
    picker = (
        (earlier[None, :] == jnp.arange(slots, dtype=jnp.int32)[:, None]) & mine[None, :]
    ).astype(jnp.float32)
    chooser = product(picker, onehot(local, old_count))
    buffer = product(chooser, old_vectors)

    packed = jnp.concatenate([reflectors, cholesky_panel, buffer], axis=0)
    packed = packed.reshape(packed.shape[0], y_width, cols).transpose(1, 0, 2)
    packed = lax.all_to_all(packed, "y", 0, 0)
    first = row_index * row_count + y_index * cols
    below = first + jnp.arange(cols, dtype=jnp.int32) >= panel
    kept = below[None, None, :] | (jnp.arange(2 * share) < share)[None, :, None]
    own_pairs = jnp.where(kept, packed[:, : 2 * share], 0.0)
    own_reflectors = packed[:, :share].reshape(-1, cols)
    own_cholesky = own_pairs[:, share:].reshape(-1, cols)
    own_slots = packed[:, 2 * share :].reshape(-1, cols)

    all_reflectors = doubled(own_reflectors, "z", HOPS)
    all_slots = doubled(own_slots, "z", HOPS)

    z_place = place_of(owner // y_width, z_index, HOPS)
    held_at = (z_place * y_width + owner % y_width) * slots + earlier
    gathered = product(onehot(held_at, slots * vec_width), all_slots)
    group = share * y_width
    turned = onehot(place_of(order // group, z_index, HOPS) * group + order % group, panel)

    with_gathered = product(own_pairs.reshape(-1, cols), gathered, (1, 1))
    with_reflectors = product(product(own_cholesky, all_reflectors, (1, 1)), turned, (1, 1))
    partial = jnp.concatenate(
        [
            with_gathered.reshape(y_width, 2 * share, panel),
            with_reflectors.reshape(y_width, share, panel),
        ],
        axis=1,
    )
    sums = summed_rows(partial)
    inner, direct, cross = (
        sums[:, :, k * share : (k + 1) * share].reshape(panel, panel) for k in range(3)
    )
    spot = (order // group) * share + (order % group) // share * (z_width * share) + order % share
    by_spot = onehot(spot, panel)
    wy_spots = product(wy_factor, by_spot)
    inverse_spots = product(panel_inverse, by_spot)

    def turns(array):
        return [array] + [
            named_permute(array, [(i, (i + d) % y_width) for i in range(y_width)])
            for d in range(1, y_width)
        ]

    reflector_blocks = turns(all_reflectors)
    gathered_blocks = turns(gathered)
    merged = []
    for block in gathered_blocks:
        merged.append(product(secular, block))
    merged, stacked = lax.optimization_barrier((jnp.stack(merged), jnp.stack(reflector_blocks)))

    projected = product(secular, inner, (1, 1))
    coeff = product(projected, wy_spots, (1, 1))
    coeff_held = product(coeff, turned)
    correction = product(secular, direct, (1, 1)) - product(coeff, cross, (1, 1))
    taken_off = product(correction, inverse_spots, (1, 1))
    where = jnp.stack([y_index, row_index]).astype(jnp.int32)
    return finished(where, merged, coeff_held, stacked, taken_off, panel_inverse)


def finished(where, merged, coeff, reflectors, taken_off, panel_inverse):
    count, vectors, cols = merged.shape
    panel = coeff.shape[1]

    def kernel(where_ref, merged_ref, coeff_ref, reflectors_ref, off_ref, inverse_ref, out_ref):
        out_ref[...] = merged_ref[0] - product(coeff_ref[...], reflectors_ref[0])

        @pl.when((pl.program_id(0) == 0) & (where_ref[1] == 0))
        def _():
            head = out_ref[:, :panel]
            out_ref[:, :panel] = product(head, inverse_ref[...], (1, 1)) - off_ref[...]

    def turned(q, where_ref):
        return (lax.rem(where_ref[0] - q + count, count), 0, 0)

    def whole(q, where_ref):
        return (0, 0)

    grid = pltpu.PrefetchScalarGridSpec(
        num_scalar_prefetch=1,
        grid=(count,),
        in_specs=[
            pl.BlockSpec((1, vectors, cols), turned),
            pl.BlockSpec(coeff.shape, whole),
            pl.BlockSpec((1, panel, cols), turned),
            pl.BlockSpec(taken_off.shape, whole),
            pl.BlockSpec(panel_inverse.shape, whole),
        ],
        out_specs=pl.BlockSpec((vectors, cols), lambda q, where_ref: (0, q)),
    )
    return pl.pallas_call(
        kernel,
        grid_spec=grid,
        out_shape=jax.ShapeDtypeStruct((vectors, count * cols), jnp.float32),
        name="finished",
    )(where, merged, coeff, reflectors, taken_off, panel_inverse)


def solution(mesh):
    split = Mesh(mesh.devices.reshape(mesh.shape["row"] // 4, 2, 2, 8, 4), ROW + VEC)

    return jax.shard_map(
        per_device,
        mesh=split,
        in_specs=(P(VEC, ROW), P(), P(VEC, None), P(VEC, ROW), P(), P(VEC, ROW), P()),
        out_specs=P(VEC, ROW),
        check_vma=False,
    )
```

```python
import jax
import jax.numpy as jnp
from jax import lax
from jax.experimental import pallas as pl
from jax.experimental.pallas import tpu as pltpu
from jax.sharding import Mesh
from jax.sharding import PartitionSpec as P


ROW = ("x", "zh", "core")
VEC = ("z", "y")
HOPS = (4, 2, 1)


def product(left, right, contract=(1, 0)):
    return lax.dot_general(
        left,
        right,
        (((contract[0],), (contract[1],)), ((), ())),
        precision=lax.Precision.HIGHEST,
        preferred_element_type=jnp.float32,
    )


def onehot(index, width):
    return (index[:, None] == jnp.arange(width, dtype=jnp.int32)[None, :]).astype(jnp.float32)


def doubled(block, axis, hops):
    width = lax.axis_size(axis)
    for hop in hops:
        other = lax.ppermute(block, axis, [(i, i ^ hop) for i in range(width)])
        block = jnp.concatenate([block, other], axis=0)
    return block


def place_of(index, mine, hops):
    apart = index ^ mine
    return sum(((apart // hop) % 2) << k for k, hop in enumerate(hops))


def spread(array, axis):
    copies = jnp.broadcast_to(array[None], (lax.axis_size(axis), *array.shape))
    return lax.all_to_all(copies, axis, 0, 0)


def summed_tiles(tiles):
    lead, tile = tiles.shape[:3], tiles.shape[3:]
    parts = lax.all_to_all(tiles.reshape(-1, *tile), ("x", "core", "y"), 0, 0)
    own = jnp.sum(parts, axis=0)
    halves = spread(own, ("zh", "z")).reshape(lax.axis_size("zh"), -1, *tile)
    column = jnp.sum(halves, axis=0)
    return spread(column, ("x", "core", "y")).reshape(*lead, -1, *tile)


def named_permute(array, pairs):
    return lax.ppermute(array, "y", pairs)


def per_device(
    old_vectors, panel_source, secular, reflectors, wy_factor, cholesky_panel, panel_inverse
):
    panel = secular.shape[1]
    old_count, row_count = old_vectors.shape
    z_width, y_width = lax.axis_size("z"), lax.axis_size("y")
    vec_width = z_width * y_width
    z_index, y_index = lax.axis_index("z"), lax.axis_index("y")
    row_index = lax.axis_index(ROW)
    share = panel // vec_width
    slots = 3 * share // 2
    cols = row_count // y_width

    owner = panel_source // old_count
    local = panel_source % old_count
    order = jnp.arange(panel, dtype=jnp.int32)
    same = (owner[:, None] == owner[None, :]) & (order[:, None] > order[None, :])
    earlier = jnp.sum(same.astype(jnp.int32), axis=1)
    mine = owner == z_index * y_width + y_index
    picker = (
        (earlier[None, :] == jnp.arange(slots, dtype=jnp.int32)[:, None]) & mine[None, :]
    ).astype(jnp.float32)
    chooser = product(picker, onehot(local, old_count))
    buffer = product(chooser, old_vectors)

    packed = jnp.concatenate([reflectors, cholesky_panel, buffer], axis=0)
    packed = packed.reshape(packed.shape[0], y_width, cols).transpose(1, 0, 2)
    packed = lax.all_to_all(packed, "y", 0, 0)
    first = row_index * row_count + y_index * cols
    below = first + jnp.arange(cols, dtype=jnp.int32) >= panel
    kept = below[None, None, :] | (jnp.arange(2 * share) < share)[None, :, None]
    own_pairs = jnp.where(kept, packed[:, : 2 * share], 0.0)
    own_reflectors = packed[:, :share].reshape(-1, cols)
    own_cholesky = own_pairs[:, share:].reshape(-1, cols)
    own_slots = packed[:, 2 * share :].reshape(-1, cols)

    all_reflectors = doubled(own_reflectors, "z", HOPS)
    all_slots = doubled(own_slots, "z", HOPS)

    z_place = place_of(owner // y_width, z_index, HOPS)
    held_at = (z_place * y_width + owner % y_width) * slots + earlier
    gathered = product(onehot(held_at, slots * vec_width), all_slots)
    group = share * y_width
    turned = onehot(place_of(order // group, z_index, HOPS) * group + order % group, panel)

    with_gathered = product(own_pairs.reshape(-1, cols), gathered, (1, 1))
    with_reflectors = product(own_cholesky, all_reflectors, (1, 1))
    with_reflectors = product(with_reflectors, turned, (1, 1))
    partial = jnp.concatenate(
        [
            with_gathered.reshape(y_width, 2 * share, panel),
            with_reflectors.reshape(y_width, share, panel),
            jnp.zeros((y_width, share, panel), jnp.float32),
        ],
        axis=1,
    )
    lanes = panel // lax.axis_size("core")
    tiles = partial.reshape(y_width, lax.axis_size("x"), share, -1, lanes).transpose(1, 3, 0, 2, 4)
    sums = summed_tiles(tiles)
    inner, direct, cross = (
        sums[k].transpose(1, 2, 3, 0, 4).reshape(panel, panel) for k in range(3)
    )
    spot = (order // group) * share + (order % group) // share * (z_width * share) + order % share
    by_spot = onehot(spot, panel)
    wy_spots = product(wy_factor, by_spot)
    inverse_spots = product(panel_inverse, by_spot)

    def turns(array):
        return [array] + [
            named_permute(array, [(i, (i + d) % y_width) for i in range(y_width)])
            for d in range(1, y_width)
        ]

    reflector_blocks = turns(all_reflectors)
    gathered_blocks = turns(gathered)
    merged = []
    for block in gathered_blocks:
        merged.append(product(secular, block))
    merged, stacked = lax.optimization_barrier((jnp.stack(merged), jnp.stack(reflector_blocks)))

    projected = product(secular, inner, (1, 1))
    coeff = product(projected, wy_spots, (1, 1))
    coeff_held = product(coeff, turned)
    correction = product(secular, direct, (1, 1)) - product(coeff, cross, (1, 1))
    taken_off = product(correction, inverse_spots, (1, 1))
    where = jnp.stack([y_index, row_index]).astype(jnp.int32)
    return finished(where, merged, coeff_held, stacked, taken_off, panel_inverse)


def finished(where, merged, coeff, reflectors, taken_off, panel_inverse):
    count, vectors, cols = merged.shape
    panel = coeff.shape[1]

    def kernel(where_ref, merged_ref, coeff_ref, reflectors_ref, off_ref, inverse_ref, out_ref):
        out_ref[...] = merged_ref[0] - product(coeff_ref[...], reflectors_ref[0])

        @pl.when((pl.program_id(0) == 0) & (where_ref[1] == 0))
        def _():
            head = out_ref[:, :panel]
            out_ref[:, :panel] = product(head, inverse_ref[...], (1, 1)) - off_ref[...]

    def turned(q, where_ref):
        return (lax.rem(where_ref[0] - q + count, count), 0, 0)

    def whole(q, where_ref):
        return (0, 0)

    grid = pltpu.PrefetchScalarGridSpec(
        num_scalar_prefetch=1,
        grid=(count,),
        in_specs=[
            pl.BlockSpec((1, vectors, cols), turned),
            pl.BlockSpec(coeff.shape, whole),
            pl.BlockSpec((1, panel, cols), turned),
            pl.BlockSpec(taken_off.shape, whole),
            pl.BlockSpec(panel_inverse.shape, whole),
        ],
        out_specs=pl.BlockSpec((vectors, cols), lambda q, where_ref: (0, q)),
    )
    return pl.pallas_call(
        kernel,
        grid_spec=grid,
        out_shape=jax.ShapeDtypeStruct((vectors, count * cols), jnp.float32),
        name="finished",
    )(where, merged, coeff, reflectors, taken_off, panel_inverse)


def solution(mesh):
    split = Mesh(mesh.devices.reshape(mesh.shape["row"] // 4, 2, 2, 8, 4), ROW + VEC)

    return jax.shard_map(
        per_device,
        mesh=split,
        in_specs=(P(VEC, ROW), P(), P(VEC, None), P(VEC, ROW), P(), P(VEC, ROW), P()),
        out_specs=P(VEC, ROW),
        check_vma=False,
    )
```

```python
import jax
import jax.numpy as jnp
from jax import lax
from jax.experimental import pallas as pl
from jax.experimental.pallas import tpu as pltpu
from jax.sharding import Mesh
from jax.sharding import PartitionSpec as P


ROW = ("x", "zh", "core")
VEC = ("z", "y")
HOPS = (4, 2, 1)


def product(left, right, contract=(1, 0)):
    return lax.dot_general(
        left,
        right,
        (((contract[0],), (contract[1],)), ((), ())),
        precision=lax.Precision.HIGHEST,
        preferred_element_type=jnp.float32,
    )


def onehot(index, width):
    return (index[:, None] == jnp.arange(width, dtype=jnp.int32)[None, :]).astype(jnp.float32)


def doubled(block, axis, hops):
    width = lax.axis_size(axis)
    for hop in hops:
        other = lax.ppermute(block, axis, [(i, i ^ hop) for i in range(width)])
        block = jnp.concatenate([block, other], axis=0)
    return block


def place_of(index, mine, hops):
    apart = index ^ mine
    return sum(((apart // hop) % 2) << k for k, hop in enumerate(hops))


def spread(array, axis):
    copies = jnp.broadcast_to(array[None], (lax.axis_size(axis), *array.shape))
    return lax.all_to_all(copies, axis, 0, 0)


def summed_tiles(tiles):
    lead, tile = tiles.shape[:3], tiles.shape[3:]
    parts = lax.all_to_all(tiles.reshape(-1, *tile), ("x", "core", "y"), 0, 0)
    own = jnp.sum(parts, axis=0)
    halves = spread(own, ("zh", "z")).reshape(lax.axis_size("zh"), -1, *tile)
    column = jnp.sum(halves, axis=0)
    return spread(column, ("x", "core", "y")).reshape(*lead, -1, *tile)


def named_permute(array, pairs):
    return lax.ppermute(array, "y", pairs)


def per_device(
    old_vectors, panel_source, secular, reflectors, wy_factor, cholesky_panel, panel_inverse
):
    panel = secular.shape[1]
    old_count, row_count = old_vectors.shape
    z_width, y_width = lax.axis_size("z"), lax.axis_size("y")
    vec_width = z_width * y_width
    z_index, y_index = lax.axis_index("z"), lax.axis_index("y")
    row_index = lax.axis_index(ROW)
    share = panel // vec_width
    slots = 3 * share // 2
    cols = row_count // y_width

    owner = panel_source // old_count
    local = panel_source % old_count
    order = jnp.arange(panel, dtype=jnp.int32)
    same = (owner[:, None] == owner[None, :]) & (order[:, None] > order[None, :])
    earlier = jnp.sum(same.astype(jnp.int32), axis=1)
    mine = owner == z_index * y_width + y_index
    picker = (
        (earlier[None, :] == jnp.arange(slots, dtype=jnp.int32)[:, None]) & mine[None, :]
    ).astype(jnp.float32)
    chooser = product(picker, onehot(local, old_count))
    buffer = product(chooser, old_vectors)

    packed = jnp.concatenate([reflectors, cholesky_panel, buffer], axis=0)
    packed = packed.reshape(packed.shape[0], y_width, cols).transpose(1, 0, 2)
    packed = lax.all_to_all(packed, "y", 0, 0)
    first = row_index * row_count + y_index * cols
    below = first + jnp.arange(cols, dtype=jnp.int32) >= panel
    kept = below[None, None, :] | (jnp.arange(2 * share) < share)[None, :, None]
    own_pairs = jnp.where(kept, packed[:, : 2 * share], 0.0)
    own_reflectors = packed[:, :share].reshape(-1, cols)
    own_cholesky = own_pairs[:, share:].reshape(-1, cols)
    own_slots = packed[:, 2 * share :].reshape(-1, cols)

    all_reflectors = doubled(own_reflectors, "z", HOPS)
    all_slots = doubled(own_slots, "z", HOPS)

    z_place = place_of(owner // y_width, z_index, HOPS)
    held_at = (z_place * y_width + owner % y_width) * slots + earlier
    gathered = product(onehot(held_at, slots * vec_width), all_slots)
    group = share * y_width
    turned = onehot(place_of(order // group, z_index, HOPS) * group + order % group, panel)

    spot = (order // group) * share + (order % group) // share * (z_width * share) + order % share
    by_spot = onehot(spot, panel)
    wy_spots = product(wy_factor, by_spot)
    inverse_spots = product(panel_inverse, by_spot)
    shaped = product(product(wy_spots, turned, (0, 0)), all_reflectors)

    with_gathered = product(own_pairs.reshape(-1, cols), gathered, (1, 1))
    with_reflectors = product(own_cholesky, all_reflectors, (1, 1))
    with_reflectors = product(with_reflectors, turned, (1, 1))
    partial = jnp.concatenate(
        [
            with_gathered.reshape(y_width, 2 * share, panel),
            with_reflectors.reshape(y_width, share, panel),
            jnp.zeros((y_width, share, panel), jnp.float32),
        ],
        axis=1,
    )
    lanes = panel // lax.axis_size("core")
    tiles = partial.reshape(y_width, lax.axis_size("x"), share, -1, lanes).transpose(1, 3, 0, 2, 4)
    sums = summed_tiles(tiles)
    inner, direct, cross = (
        sums[k].transpose(1, 2, 3, 0, 4).reshape(panel, panel) for k in range(3)
    )

    def turns(array):
        return [array] + [
            named_permute(array, [(i, (i + d) % y_width) for i in range(y_width)])
            for d in range(1, y_width)
        ]

    shaped_blocks = turns(shaped)
    gathered_blocks = turns(gathered)
    merged = []
    for block in gathered_blocks:
        merged.append(product(secular, block))
    stacked = jnp.stack(shaped_blocks)
    high = lax.reduce_precision(stacked, 8, 7)
    low = (stacked - high).astype(jnp.bfloat16)
    merged, high, low = lax.optimization_barrier(
        (jnp.stack(merged), high.astype(jnp.bfloat16), low)
    )

    projected = product(secular, inner, (1, 1))
    coeff = product(projected, wy_spots, (1, 1))
    correction = product(secular, direct, (1, 1)) - product(coeff, cross, (1, 1))
    taken_off = product(correction, inverse_spots, (1, 1))
    where = jnp.stack([y_index, row_index]).astype(jnp.int32)
    return finished(where, merged, projected, high, low, taken_off, panel_inverse)


def finished(where, merged, factor, high, low, taken_off, panel_inverse):
    count, vectors, cols = merged.shape
    panel = factor.shape[1]

    def once(left, right):
        return jnp.dot(left, right, preferred_element_type=jnp.float32)

    def kernel(where_ref, merged_ref, factor_ref, high_ref, low_ref, off_ref, inverse_ref, out_ref):
        left = factor_ref[...]
        left_high = left.astype(jnp.bfloat16)
        left_low = (left - left_high.astype(jnp.float32)).astype(jnp.bfloat16)
        taken = once(left_high, low_ref[0]) + once(left_low, high_ref[0])
        taken = taken + once(left_high, high_ref[0])
        out_ref[...] = merged_ref[0] - taken

        @pl.when((pl.program_id(0) == 0) & (where_ref[1] == 0))
        def _():
            head = out_ref[:, :panel]
            out_ref[:, :panel] = product(head, inverse_ref[...], (1, 1)) - off_ref[...]

    def turned(q, where_ref):
        return (lax.rem(where_ref[0] - q + count, count), 0, 0)

    def whole(q, where_ref):
        return (0, 0)

    grid = pltpu.PrefetchScalarGridSpec(
        num_scalar_prefetch=1,
        grid=(count,),
        in_specs=[
            pl.BlockSpec((1, vectors, cols), turned),
            pl.BlockSpec(factor.shape, whole),
            pl.BlockSpec((1, panel, cols), turned),
            pl.BlockSpec((1, panel, cols), turned),
            pl.BlockSpec(taken_off.shape, whole),
            pl.BlockSpec(panel_inverse.shape, whole),
        ],
        out_specs=pl.BlockSpec((vectors, cols), lambda q, where_ref: (0, q)),
    )
    return pl.pallas_call(
        kernel,
        grid_spec=grid,
        out_shape=jax.ShapeDtypeStruct((vectors, count * cols), jnp.float32),
        name="finished",
    )(where, merged, factor, high, low, taken_off, panel_inverse)


def solution(mesh):
    split = Mesh(mesh.devices.reshape(mesh.shape["row"] // 4, 2, 2, 8, 4), ROW + VEC)

    return jax.shard_map(
        per_device,
        mesh=split,
        in_specs=(P(VEC, ROW), P(), P(VEC, None), P(VEC, ROW), P(), P(VEC, ROW), P()),
        out_specs=P(VEC, ROW),
        check_vma=False,
    )
```

```python
import jax
import jax.numpy as jnp
from jax import lax
from jax.experimental import pallas as pl
from jax.experimental.pallas import tpu as pltpu
from jax.sharding import Mesh
from jax.sharding import PartitionSpec as P


ROW = ("x", "zh", "core")
VEC = ("z", "y")
HOPS = (4, 2, 1)


def product(left, right, contract=(1, 0)):
    return lax.dot_general(
        left,
        right,
        (((contract[0],), (contract[1],)), ((), ())),
        precision=lax.Precision.HIGHEST,
        preferred_element_type=jnp.float32,
    )


def onehot(index, width):
    return (index[:, None] == jnp.arange(width, dtype=jnp.int32)[None, :]).astype(jnp.float32)


def doubled(block, axis, hops):
    width = lax.axis_size(axis)
    for hop in hops:
        other = lax.ppermute(block, axis, [(i, i ^ hop) for i in range(width)])
        block = jnp.concatenate([block, other], axis=0)
    return block


def place_of(index, mine, hops):
    apart = index ^ mine
    return sum(((apart // hop) % 2) << k for k, hop in enumerate(hops))


def spread(array, axis):
    copies = jnp.broadcast_to(array[None], (lax.axis_size(axis), *array.shape))
    return lax.all_to_all(copies, axis, 0, 0)


def summed_tiles(tiles):
    lead, tile = tiles.shape[:3], tiles.shape[3:]
    parts = lax.all_to_all(tiles.reshape(-1, *tile), ("x", "core", "y"), 0, 0)
    own = jnp.sum(parts, axis=0)
    halves = spread(own, ("zh", "z")).reshape(lax.axis_size("zh"), -1, *tile)
    column = jnp.sum(halves, axis=0)
    return spread(column, ("x", "core", "y")).reshape(*lead, -1, *tile)


def named_permute(array, pairs):
    return lax.ppermute(array, "y", pairs)


def per_device(
    old_vectors, panel_source, secular, reflectors, wy_factor, cholesky_panel, panel_inverse
):
    panel = secular.shape[1]
    old_count, row_count = old_vectors.shape
    z_width, y_width = lax.axis_size("z"), lax.axis_size("y")
    vec_width = z_width * y_width
    z_index, y_index = lax.axis_index("z"), lax.axis_index("y")
    row_index = lax.axis_index(ROW)
    share = panel // vec_width
    slots = 3 * share // 2
    cols = row_count // y_width

    owner = panel_source // old_count
    local = panel_source % old_count
    order = jnp.arange(panel, dtype=jnp.int32)
    same = (owner[:, None] == owner[None, :]) & (order[:, None] > order[None, :])
    earlier = jnp.sum(same.astype(jnp.int32), axis=1)
    mine = owner == z_index * y_width + y_index
    picker = (
        (earlier[None, :] == jnp.arange(slots, dtype=jnp.int32)[:, None]) & mine[None, :]
    ).astype(jnp.float32)
    chooser = product(picker, onehot(local, old_count))
    buffer = product(chooser, old_vectors)

    packed = jnp.concatenate([reflectors, cholesky_panel, buffer], axis=0)
    packed = packed.reshape(packed.shape[0], y_width, cols).transpose(1, 0, 2)
    packed = lax.all_to_all(packed, "y", 0, 0)
    first = row_index * row_count + y_index * cols
    below = first + jnp.arange(cols, dtype=jnp.int32) >= panel
    kept = below[None, None, :] | (jnp.arange(2 * share) < share)[None, :, None]
    own_pairs = jnp.where(kept, packed[:, : 2 * share], 0.0)
    own_reflectors = packed[:, :share].reshape(-1, cols)
    own_cholesky = own_pairs[:, share:].reshape(-1, cols)
    own_slots = packed[:, 2 * share :].reshape(-1, cols)

    all_reflectors = doubled(own_reflectors, "z", HOPS)
    all_slots = doubled(own_slots, "z", HOPS)

    z_place = place_of(owner // y_width, z_index, HOPS)
    held_at = (z_place * y_width + owner % y_width) * slots + earlier
    gathered = product(onehot(held_at, slots * vec_width), all_slots)
    group = share * y_width
    turned = onehot(place_of(order // group, z_index, HOPS) * group + order % group, panel)

    spot = (order // group) * share + (order % group) // share * (z_width * share) + order % share
    by_spot = onehot(spot, panel)
    wy_spots = product(wy_factor, by_spot)
    inverse_spots = product(panel_inverse, by_spot)
    shaped = product(product(wy_spots, turned, (0, 0)), all_reflectors)

    with_gathered = product(own_pairs.reshape(-1, cols), gathered, (1, 1))
    with_reflectors = product(own_cholesky, all_reflectors, (1, 1))
    with_reflectors = product(with_reflectors, turned, (1, 1))
    partial = jnp.concatenate(
        [
            with_gathered.reshape(y_width, 2 * share, panel),
            with_reflectors.reshape(y_width, share, panel),
            jnp.zeros((y_width, share, panel), jnp.float32),
        ],
        axis=1,
    )
    lanes = panel // lax.axis_size("core")
    tiles = partial.reshape(y_width, lax.axis_size("x"), share, -1, lanes).transpose(1, 3, 0, 2, 4)
    sums = summed_tiles(tiles)
    inner, direct, cross = (
        sums[k].transpose(1, 2, 3, 0, 4).reshape(panel, panel) for k in range(3)
    )

    def turns(array):
        return [array] + [
            named_permute(array, [(i, (i + d) % y_width) for i in range(y_width)])
            for d in range(1, y_width)
        ]

    shaped_blocks = turns(shaped)
    gathered_blocks = turns(gathered)
    merged = []
    for block in gathered_blocks:
        merged.append(product(secular, block))
    stacked = jnp.stack(shaped_blocks)
    high = lax.reduce_precision(stacked, 8, 7)
    low = (stacked - high).astype(jnp.bfloat16)
    merged, high, low = lax.optimization_barrier(
        (jnp.stack(merged), high.astype(jnp.bfloat16), low)
    )

    where = jnp.stack([y_index, row_index]).astype(jnp.int32)
    small = (secular, inner, direct, cross, wy_spots, inverse_spots, panel_inverse)
    return finished(where, merged, high, low, small)


def finished(where, merged, high, low, small):
    count, vectors, cols = merged.shape
    panel = high.shape[1]

    def once(left, right):
        return jnp.dot(left, right, preferred_element_type=jnp.float32)

    def kernel(where_ref, merged_ref, high_ref, low_ref, *refs):
        secular_ref, inner_ref, direct_ref, cross_ref, wy_ref, spots_ref, inverse_ref = refs[:7]
        out_ref, factor_ref, factor_high, factor_low = refs[7:]
        step = pl.program_id(0)

        @pl.when(step == 0)
        def _():
            factor = product(secular_ref[...], inner_ref[...], (1, 1))
            rounded = factor.astype(jnp.bfloat16)
            factor_ref[...] = factor
            factor_high[...] = rounded
            factor_low[...] = (factor - rounded.astype(jnp.float32)).astype(jnp.bfloat16)

        block = lax.rem(where_ref[0] - step + count, count)
        taken = once(factor_high[...], low_ref[block]) + once(factor_low[...], high_ref[block])
        taken = taken + once(factor_high[...], high_ref[block])
        out_ref[...] = merged_ref[block] - taken

        @pl.when((step == 0) & (where_ref[1] == 0))
        def _():
            coeff = product(factor_ref[...], wy_ref[...], (1, 1))
            correction = product(secular_ref[...], direct_ref[...], (1, 1))
            correction = correction - product(coeff, cross_ref[...], (1, 1))
            solved = product(out_ref[:, :panel], inverse_ref[...], (1, 1))
            out_ref[:, :panel] = solved - product(correction, spots_ref[...], (1, 1))

    operands = [
        pltpu.with_memory_space_constraint(array, pltpu.VMEM)
        for array in (merged, high, low, *small)
    ]
    grid = pltpu.PrefetchScalarGridSpec(
        num_scalar_prefetch=1,
        grid=(count,),
        in_specs=[pl.BlockSpec(memory_space=pltpu.VMEM)] * len(operands),
        out_specs=pl.BlockSpec((vectors, cols), lambda q, where_ref: (0, q)),
        scratch_shapes=[
            pltpu.VMEM((vectors, panel), jnp.float32),
            pltpu.VMEM((vectors, panel), jnp.bfloat16),
            pltpu.VMEM((vectors, panel), jnp.bfloat16),
        ],
    )
    return pl.pallas_call(
        kernel,
        grid_spec=grid,
        out_shape=jax.ShapeDtypeStruct((vectors, count * cols), jnp.float32),
        compiler_params=pltpu.CompilerParams(vmem_limit_bytes=16 * 2**20),
        name="finished",
    )(where, *operands)


def solution(mesh):
    split = Mesh(mesh.devices.reshape(mesh.shape["row"] // 4, 2, 2, 8, 4), ROW + VEC)

    return jax.shard_map(
        per_device,
        mesh=split,
        in_specs=(P(VEC, ROW), P(), P(VEC, None), P(VEC, ROW), P(), P(VEC, ROW), P()),
        out_specs=P(VEC, ROW),
        check_vma=False,
    )
```
